128 devices in a mesh: pair: 8 (over x, core), ep: 16 (over z, y).
Axes of the slice: x: 4, y: 4, z: 4, core: 2. Of those that a mesh axis runs over, the one named last changes fastest.
Arguments:
- tokens: bfloat16 [32768, 4096], P(('pair', 'ep')), may hold values from -6 to 6
- expert_of: int32 [32768, 1], P(('pair', 'ep')), may hold values from 0 to 127, as said below
- w_gate: bfloat16 [128, 4096, 768], P(('pair', 'ep')), may hold values from -0.09375 to 0.09375
- w_up: bfloat16 [128, 4096, 768], P(('pair', 'ep')), may hold values from -0.09375 to 0.09375
- w_down: bfloat16 [128, 768, 4096], P(('pair', 'ep')), may hold values from -0.21875 to 0.21875
Outputs:
- mixed: bfloat16 [32768, 4096], P(('pair', 'ep'))
The draws below stay inside these ranges and needn't reach their ends.
Inputs may be any that keep to these rules, and one draw needn't show every extreme that they name: `expert_of`: the rows of one device (aligned blocks of 256 tokens) name no expert more than 3 times; in every draw one expert, drawn from the seed, is named exactly 3 times in every device's rows.
All inputs are finite; a program needn't handle non-finite values.
Results may differ from the reference program's by a relative error of at most 0.005.
Values may be sent and summed in bfloat16 or wider, within the bound.
A program may use at most 128 MiB of HBM per device.

```python
import jax
import jax.numpy as jnp
from jax import lax

D = 4096
FF = 768
TOK_DEV = 256
EXPERTS = 128
CAP = 3
TOKENS = 32768


def draw_expert_of(key, part):
    blocks = TOKENS // TOK_DEV
    hottest = jax.random.randint(jax.random.fold_in(key, 7), (), 0, EXPERTS).astype(jnp.int32)
    block_keys = jax.random.split(jax.random.fold_in(key, 11), blocks)

    def one_block(block_key):
        first_key, second_key = jax.random.split(block_key)
        others = jnp.repeat(jnp.arange(EXPERTS - 1, dtype=jnp.int32), CAP)
        others = jax.random.permutation(first_key, others)[:TOK_DEV - CAP]
        others = others + (others >= hottest).astype(jnp.int32)
        block_rows = jnp.concatenate([jnp.full((CAP,), hottest, jnp.int32), others])
        return jax.random.permutation(second_key, block_rows)
    return jax.vmap(one_block)(block_keys).reshape(TOKENS, 1).astype(jnp.int32)


def steps_of(stream_key, dims, shards, least, high):
    def one(dim, blocks):
        steps = jax.random.uniform(jax.random.fold_in(jax.random.fold_in(stream_key, 6), dim), (blocks,), jnp.float32, least / len(shards), high / len(shards))
        return jnp.repeat(jnp.exp(steps), dims[dim] // blocks).reshape((-1,) + (1,) * (len(dims) - dim - 1))

    level = one(*shards[0])
    for cut in shards[1:]:
        level = level * one(*cut)
    return level


def normal_values(stream_key, extent, scale, bound, cuts=(), kind=jnp.bfloat16):
    values = scale * jax.random.normal(stream_key, extent, jnp.float32)
    if cuts:
        values = values * steps_of(stream_key, extent, cuts, -0.22, 0.18)
    return jnp.clip(values, -bound, bound).astype(kind)


def setup_inputs(seed: int = 0) -> dict:
    keys = jax.random.split(jax.random.key(seed), 6)
    return {
        "tokens": normal_values(keys[0], (TOKENS, D), 1.0, 6.0, ((0, 128),)),
        "expert_of": draw_expert_of(jax.random.fold_in(keys[5], 71), 0),
        "w_gate": normal_values(keys[2], (EXPERTS, D, FF), D ** -0.5, 0.09375, ((0, 128),)),
        "w_up": normal_values(keys[3], (EXPERTS, D, FF), D ** -0.5, 0.09375, ((0, 128),)),
        "w_down": normal_values(keys[4], (EXPERTS, FF, D), FF ** -0.5, 0.21875, ((0, 128),)),
    }


def reference(tokens, expert_of, w_gate, w_up, w_down):
    routed = expert_of[:, 0].astype(jnp.int32)
    row_limit = EXPERTS * CAP
    sorted_rows = jnp.argsort(routed, stable=True).astype(jnp.int32)
    expert_load = jnp.sum((routed[:, None] == jnp.arange(EXPERTS, dtype=jnp.int32)[None, :]).astype(jnp.int32), axis=0).astype(jnp.int32)
    offsets = (jnp.cumsum(expert_load) - expert_load).astype(jnp.int32)
    padded_order = jnp.concatenate([sorted_rows, jnp.full((row_limit,), TOKENS, jnp.int32)])

    def per_expert(mixed_sofar, expert):
        picked = lax.dynamic_slice(padded_order, (offsets[expert].astype(jnp.int32),), (row_limit,))
        is_live = jnp.arange(row_limit, dtype=jnp.int32) < expert_load[expert]
        picked = jnp.where(is_live, picked, TOKENS).astype(jnp.int32)
        gathered = jnp.take(tokens, jnp.minimum(picked, TOKENS - 1), axis=0)
        gate_proj = jnp.dot(gathered, w_gate[expert], preferred_element_type=jnp.float32)
        up_proj = jnp.dot(gathered, w_up[expert], preferred_element_type=jnp.float32)
        hidden = (jax.nn.silu(gate_proj) * up_proj).astype(jnp.bfloat16)
        result = jnp.dot(hidden, w_down[expert], preferred_element_type=jnp.float32).astype(jnp.bfloat16)
        return mixed_sofar.at[picked].set(result, mode="drop"), None

    start = jnp.zeros((TOKENS, D), jnp.bfloat16)
    mixed, _ = lax.scan(per_expert, start, jnp.arange(EXPERTS, dtype=jnp.int32))
    return mixed
```

```python
import functools

import jax
import jax.numpy as jnp
from jax import lax
from jax.experimental import pallas as pl
from jax.experimental.pallas import tpu as pltpu
from jax.sharding import PartitionSpec as P

MESH = pl.DeviceIdType.MESH
BF16 = jnp.bfloat16
F32 = jnp.float32

DEVICES = 128
CAP = 3
STEP = 37
UNSTEP = pow(STEP, -1, DEVICES)
CUT, WIDE = 16, 256
GROUPS = ((0, 64), (64, 64))


def dims():
    pair, ep = lax.axis_index("pair"), lax.axis_index("ep")
    return pair // 2, pair % 2, ep // 4, ep % 4


def peer(step, sign):
    off = (step * STEP) % DEVICES
    x, core, z, y = dims()
    px = (x + 4 + sign * (off // 32)) % 4
    pc = (core + off // 16) % 2
    pz = (z + 4 + sign * ((off // 4) % 4)) % 4
    py = (y + 4 + sign * (off % 4)) % 4
    return px * 2 + pc, pz * 4 + py


def step_of(expert):
    x, core, z, y = dims()
    dx = (expert // 32 + 4 - x) % 4
    dc = ((expert // 16) % 2 + core) % 2
    dz = ((expert // 4) % 4 + 4 - z) % 4
    dy = (expert % 4 + 4 - y) % 4
    return ((dx * 32 + dc * 16 + dz * 4 + dy) * UNSTEP) % DEVICES


def kernel(
    expert_ref, tok_hbm, wg_hbm, wu_hbm, wd_hbm, mixed_ref,
    tok, wg, wu, wd, rows, hid, pick, place, turn, outgoing, parcel, result, returned,
    tok_sem, w_sem, send_sem, there_sem, back_send_sem, back_sem,
):
    barrier = pltpu.get_barrier_semaphore()

    @pl.loop(1, DEVICES)
    def _(k):
        pl.semaphore_signal(barrier, inc=1, device_id=peer(k, 1), device_id_type=MESH)

    tok_copy = pltpu.make_async_copy(tok_hbm, tok, tok_sem)
    tok_copy.start()
    w_copies = [
        pltpu.make_async_copy(src.at[0], dst, w_sem.at[i])
        for i, (src, dst) in enumerate(((wg_hbm, wg), (wu_hbm, wu), (wd_hbm, wd)))
    ]
    for copy in w_copies:
        copy.start()

    count = tok.shape[0]
    slots = DEVICES * CAP
    column = expert_ref[...]
    down = lax.broadcasted_iota(jnp.int32, (count, count), 0)
    across = lax.broadcasted_iota(jnp.int32, (count, count), 1)
    row = jnp.sum(jnp.where(down == across, column, 0), axis=0, keepdims=True)
    same = column == row
    row_rank = jnp.sum(jnp.where(same & (down < across), 1, 0), axis=0, keepdims=True)
    col_rank = jnp.sum(jnp.where(same & (across < down), 1, 0), axis=1, keepdims=True)
    row_slot = step_of(row) * CAP + row_rank
    col_slot = step_of(column) * CAP + col_rank
    pick[...] = jnp.where(
        lax.broadcasted_iota(jnp.int32, (slots, count), 0) == row_slot, 1.0, 0.0
    ).astype(BF16)
    place[...] = jnp.where(
        lax.broadcasted_iota(jnp.int32, (count, slots), 1) == col_slot, 1.0, 0.0
    ).astype(BF16)
    n = CUT * CUT
    turn_row = lax.broadcasted_iota(jnp.int32, (n, n), 0)
    turn_col = lax.broadcasted_iota(jnp.int32, (n, n), 1)
    turn[...] = jnp.where(
        (turn_row // CUT == turn_col % CUT) & (turn_row % CUT == turn_col // CUT), 1.0, 0.0
    ).astype(BF16)

    def pack(src, dst, block):
        at = pl.multiple_of(block * CUT, CUT)
        cut = jnp.concatenate(
            [src[pl.ds(at, CUT), c * WIDE : (c + 1) * WIDE] for c in range(CUT)], axis=0
        )
        turned = jnp.dot(turn[...], cut, preferred_element_type=F32).astype(BF16)
        dst[pl.ds(pl.multiple_of(block * n, n), n), :] = turned

    def unpack(src, dst, block):
        at = pl.multiple_of(block * CUT, CUT)
        cut = src[pl.ds(pl.multiple_of(block * n, n), n), :]
        turned = jnp.dot(turn[...], cut, preferred_element_type=F32).astype(BF16)
        for c in range(CUT):
            dst[pl.ds(at, CUT), c * WIDE : (c + 1) * WIDE] = turned[c * CUT : (c + 1) * CUT, :]

    parcel_rows = CAP * CUT

    def span(step, steps=1):
        return pl.ds(pl.multiple_of(step * parcel_rows, parcel_rows), steps * parcel_rows)

    def there(k, sem):
        return pltpu.make_async_remote_copy(
            src_ref=outgoing.at[span(k)], dst_ref=parcel.at[span(k)],
            send_sem=send_sem, recv_sem=sem, device_id=peer(k, 1), device_id_type=MESH,
        )

    def back(k, sem):
        return pltpu.make_async_remote_copy(
            src_ref=result.at[span(k)], dst_ref=returned.at[span(k)],
            send_sem=back_send_sem, recv_sem=sem, device_id=peer(k, -1), device_id_type=MESH,
        )

    tok_copy.wait()

    @pl.loop(0, CUT)
    def _(c):
        at = pl.ds(pl.multiple_of(c * WIDE, WIDE), WIDE)
        rows[:, at] = jnp.dot(pick[...], tok[:, at], preferred_element_type=F32).astype(BF16)

    unit = 16
    blocks = unit * CAP // CUT
    units = DEVICES // unit

    def pack_unit(u):
        @pl.loop(0, blocks)
        def _(b):
            pack(rows, outgoing, u * blocks + b)

    for g, (first, steps) in enumerate(GROUPS):
        for u in range(first // unit, (first + steps) // unit):
            if u == 0:
                pack_unit(0)
                pl.semaphore_wait(barrier, DEVICES - 1)
            if u + 1 < units:
                pack_unit(u + 1)

            @pl.loop(max(u * unit, 1), (u + 1) * unit)
            def _(k):
                there(k, there_sem.at[g]).start()

    parcel[: parcel_rows, :] = outgoing[: parcel_rows, :]

    for g, (first, steps) in enumerate(GROUPS):
        lo = max(first, 1)
        got = span(lo, first + steps - lo)
        pltpu.make_async_remote_copy(
            src_ref=outgoing.at[got], dst_ref=parcel.at[got], send_sem=send_sem,
            recv_sem=there_sem.at[g], device_id=peer(1, 1), device_id_type=MESH,
        ).wait_recv()
        r0, m = first * CAP, steps * CAP

        @pl.loop(r0 // CUT, (r0 + m) // CUT)
        def _(b):
            unpack(parcel, rows, b)

        if g == 0:
            w_copies[0].wait()
            w_copies[1].wait()

        @pl.loop(0, wg.shape[1] // WIDE)
        def _(j):
            at = pl.ds(pl.multiple_of(j * WIDE, WIDE), WIDE)
            x = rows[r0 : r0 + m, :]
            gate = jnp.dot(x, wg[:, at], preferred_element_type=F32)
            up = jnp.dot(x, wu[:, at], preferred_element_type=F32)
            hid[:m, at] = (gate / (1.0 + jnp.exp(-gate)) * up).astype(BF16)

        if g == 0:
            w_copies[2].wait()

        @pl.loop(0, CUT)
        def _(c):
            at = pl.ds(pl.multiple_of(c * WIDE, WIDE), WIDE)
            rows[r0 : r0 + m, at] = jnp.dot(
                hid[:m, :], wd[:, at], preferred_element_type=F32
            ).astype(BF16)

        @pl.loop(r0 // CUT, (r0 + m) // CUT)
        def _(b):
            pack(rows, result, b)

        @pl.loop(lo, first + steps)
        def _(k):
            back(k, back_sem.at[g]).start()

        if g == 0:
            returned[: parcel_rows, :] = result[: parcel_rows, :]

    for g, (first, steps) in enumerate(GROUPS):
        lo = max(first, 1)
        got = span(lo, first + steps - lo)
        pltpu.make_async_remote_copy(
            src_ref=result.at[got], dst_ref=returned.at[got], send_sem=back_send_sem,
            recv_sem=back_sem.at[g], device_id=peer(1, 1), device_id_type=MESH,
        ).wait_recv()

        @pl.loop(first * CAP // CUT, (first + steps) * CAP // CUT)
        def _(b):
            unpack(returned, rows, b)

    @pl.loop(0, CUT)
    def _(c):
        at = pl.ds(pl.multiple_of(c * WIDE, WIDE), WIDE)
        mixed_ref[:, at] = jnp.dot(
            place[...], rows[:, at], preferred_element_type=F32
        ).astype(BF16)

    sent = span(1, DEVICES - 1)
    for src, dst, sem in ((outgoing, parcel, send_sem), (result, returned, back_send_sem)):
        pltpu.make_async_remote_copy(
            src_ref=src.at[sent], dst_ref=dst.at[sent], send_sem=sem,
            recv_sem=there_sem.at[0], device_id=peer(1, 1), device_id_type=MESH,
        ).wait_send()


def shards(tokens, expert_of, w_gate, w_up, w_down):
    count, width = tokens.shape
    hidden = w_gate.shape[2]
    slots = DEVICES * CAP
    packed = pltpu.VMEM((slots * CUT, WIDE), BF16)
    hbm = pl.BlockSpec(memory_space=pl.ANY)
    vmem = pl.BlockSpec(memory_space=pltpu.VMEM)
    return pl.pallas_call(
        kernel,
        out_shape=jax.ShapeDtypeStruct((count, width), BF16),
        in_specs=[vmem, hbm, hbm, hbm, hbm],
        out_specs=vmem,
        scratch_shapes=[
            pltpu.VMEM((count, width), BF16),
            pltpu.VMEM((width, hidden), BF16),
            pltpu.VMEM((width, hidden), BF16),
            pltpu.VMEM((hidden, width), BF16),
            pltpu.VMEM((slots, width), BF16),
            pltpu.VMEM((max(s for _, s in GROUPS) * CAP, hidden), BF16),
            pltpu.VMEM((slots, count), BF16),
            pltpu.VMEM((count, slots), BF16),
            pltpu.VMEM((CUT * CUT, CUT * CUT), BF16),
            packed, packed, packed, packed,
            pltpu.SemaphoreType.DMA,
            pltpu.SemaphoreType.DMA((3,)),
            pltpu.SemaphoreType.DMA,
            pltpu.SemaphoreType.DMA((len(GROUPS),)),
            pltpu.SemaphoreType.DMA,
            pltpu.SemaphoreType.DMA((len(GROUPS),)),
        ],
        compiler_params=pltpu.CompilerParams(
            collective_id=0, has_side_effects=True, vmem_limit_bytes=56 * 1024 * 1024
        ),
        name="expert_exchange",
    )(expert_of, tokens, w_gate, w_up, w_down)


def solution(mesh):
    rows = P(("pair", "ep"), None)
    blocks = P(("pair", "ep"), None, None)
    return jax.shard_map(
        shards, mesh=mesh, in_specs=(rows, rows, blocks, blocks, blocks), out_specs=rows,
        check_vma=False,
    )
```

```python
import jax
import jax.numpy as jnp
from jax import lax
from jax.experimental import pallas as pl
from jax.experimental.pallas import tpu as pltpu
from jax.sharding import PartitionSpec as P

MESH = pl.DeviceIdType.MESH
BF16 = jnp.bfloat16
F32 = jnp.float32

DEVICES = 128
CAP = 3
STEP = 37
UNSTEP = pow(STEP, -1, DEVICES)
CUT, WIDE = 16, 256
UNIT = 32
SLOTS = UNIT * CAP
BLOCKS = SLOTS // CUT
UNITS = DEVICES // UNIT
GROUPS = ((0, 1), (2, 3))
LANDINGS = ((0, 1), (2,), (3,))
SPREAD = 1024


def step_of(expert, x, core, z, y):
    dx = (expert // 32 + 4 - x) % 4
    dc = ((expert // 16) % 2 + core) % 2
    dz = ((expert // 4) % 4 + 4 - z) % 4
    dy = (expert % 4 + 4 - y) % 4
    return ((dx * 32 + dc * 16 + dz * 4 + dy) * UNSTEP) % DEVICES


def kernel(
    expert_hbm, tok_hbm, wg_hbm, wu_hbm, wd_hbm, mixed_ref,
    expert, tok, wg, wu, wd, rows, hid, place, turn, outgoing, parcel, result, returned,
    expert_sem, tok_sem, w_sem, send_sem, there_sem, back_send_sem, back_sem,
):
    pair, ep = lax.axis_index("pair"), lax.axis_index("ep")
    x, core, z, y = pair // 2, pair % 2, ep // 4, ep % 4
    pairs = [((x + d // 2) % 4) * 2 + (core + d % 2) % 2 for d in range(8)]
    eps = [((z + d // 4) % 4) * 4 + (y + d % 4) % 4 for d in range(16)]

    def peer(step, sign):
        off = (step * STEP) % DEVICES
        dx, dc, dz, dy = off // 32, (off // 16) % 2, (off // 4) % 4, off % 4
        return pairs[(sign * dx) % 4 * 2 + dc], eps[(sign * dz) % 4 * 4 + (sign * dy) % 4]

    expert_copy = pltpu.make_async_copy(expert_hbm, expert, expert_sem)
    expert_copy.start()
    tok_copy = pltpu.make_async_copy(tok_hbm, tok, tok_sem)
    tok_copy.start()
    barrier = pltpu.get_barrier_semaphore()
    for k in range(1, DEVICES):
        pl.semaphore_signal(barrier, inc=1, device_id=peer(k, 1), device_id_type=MESH)

    count = tok.shape[0]
    expert_copy.wait()
    row = expert[...]
    down = lax.broadcasted_iota(jnp.int32, (count, count), 0)
    across = lax.broadcasted_iota(jnp.int32, (count, count), 1)
    column = jnp.sum(jnp.where(down == across, row, 0), axis=1, keepdims=True)
    same = column == row
    row_rank = jnp.sum(jnp.where(same & (down < across), 1, 0), axis=0, keepdims=True)
    row_slot = step_of(row, x, core, z, y) * CAP + row_rank
    n = CUT * CUT
    turn_row = lax.broadcasted_iota(jnp.int32, (n, n), 0)
    turn_col = lax.broadcasted_iota(jnp.int32, (n, n), 1)
    turn[...] = jnp.where(
        (turn_row // CUT == turn_col % CUT) & (turn_row % CUT == turn_col // CUT), 1.0, 0.0
    ).astype(BF16)

    def pack(src, dst, unit):
        for b in range(unit * BLOCKS, (unit + 1) * BLOCKS):
            cut = jnp.concatenate(
                [src[b * CUT : (b + 1) * CUT, c * WIDE : (c + 1) * WIDE] for c in range(CUT)],
                axis=0,
            )
            turned = jnp.dot(turn[...], cut, preferred_element_type=F32).astype(BF16)
            dst[b * n : (b + 1) * n, :] = turned

    def unpack(src, dst, unit):
        for b in range(unit * BLOCKS, (unit + 1) * BLOCKS):
            cut = src[b * n : (b + 1) * n, :]
            turned = jnp.dot(turn[...], cut, preferred_element_type=F32).astype(BF16)
            for c in range(CUT):
                dst[b * CUT : (b + 1) * CUT, c * WIDE : (c + 1) * WIDE] = turned[
                    c * CUT : (c + 1) * CUT, :
                ]

    def spread(body):
        @pl.loop(0, tok.shape[1] // SPREAD)
        def _(c):
            body(pl.ds(pl.multiple_of(c * SPREAD, SPREAD), SPREAD))

    parcel_rows = CAP * CUT

    def span(step, steps=1):
        return pl.ds(step * parcel_rows, steps * parcel_rows)

    def there(k, steps=1):
        return pltpu.make_async_remote_copy(
            src_ref=outgoing.at[span(k, steps)], dst_ref=parcel.at[span(k, steps)],
            send_sem=send_sem, recv_sem=there_sem.at[[k // UNIT in g for g in GROUPS].index(True)],
            device_id=peer(k, 1), device_id_type=MESH,
        )

    def back(k, steps=1):
        return pltpu.make_async_remote_copy(
            src_ref=result.at[span(k, steps)], dst_ref=returned.at[span(k, steps)],
            send_sem=back_send_sem,
            recv_sem=back_sem.at[[k // UNIT in g for g in LANDINGS].index(True)],
            device_id=peer(k, -1), device_id_type=MESH,
        )

    def send(copy, unit):
        for k in range(max(unit * UNIT, 1), (unit + 1) * UNIT):
            copy(k).start()

    def await_units(copy, units):
        lo = max(units[0] * UNIT, 1)
        copy(lo, (units[-1] + 1) * UNIT - lo).wait_recv()

    def select(unit):
        pick = jnp.where(
            lax.broadcasted_iota(jnp.int32, (SLOTS, count), 0) + unit * SLOTS == row_slot, 1.0, 0.0
        ).astype(BF16)

        @spread
        def _(at):
            rows[unit * SLOTS : (unit + 1) * SLOTS, at] = jnp.dot(
                pick, tok[:, at], preferred_element_type=F32
            ).astype(BF16)

    tok_copy.wait()
    for u in range(UNITS):
        select(u)
        pack(rows, outgoing, u)
        if u == 0:
            pl.semaphore_wait(barrier, DEVICES - 1)
        else:
            send(there, u - 1)
    send(there, UNITS - 1)
    parcel[:parcel_rows, :] = outgoing[:parcel_rows, :]

    w_copies = [
        pltpu.make_async_copy(src.at[0], dst, w_sem.at[i])
        for i, (src, dst) in enumerate(((wg_hbm, wg), (wu_hbm, wu), (wd_hbm, wd)))
    ]
    for copy in w_copies:
        copy.start()

    col_rank = jnp.sum(jnp.where(same & (across < down), 1, 0), axis=1, keepdims=True)
    col_slot = step_of(column, x, core, z, y) * CAP + col_rank
    place[...] = jnp.where(
        lax.broadcasted_iota(jnp.int32, (count, DEVICES * CAP), 1) == col_slot, 1.0, 0.0
    ).astype(BF16)
    for copy in w_copies:
        copy.wait()

    for units in GROUPS:
        await_units(there, units)
        for u in units:
            unpack(parcel, rows, u)
        held = slice(units[0] * SLOTS, (units[-1] + 1) * SLOTS)
        for j in range(0, wg.shape[1], WIDE):
            arrived = rows[held, :]
            gate = jnp.dot(arrived, wg[:, j : j + WIDE], preferred_element_type=F32)
            up = jnp.dot(arrived, wu[:, j : j + WIDE], preferred_element_type=F32)
            hid[held, j : j + WIDE] = (gate / (1.0 + jnp.exp(-gate)) * up).astype(BF16)

        @spread
        def _(at):
            rows[held, at] = jnp.dot(hid[held, :], wd[:, at], preferred_element_type=F32).astype(BF16)

        for i, u in enumerate(units):
            pack(rows, result, u)
            if i:
                send(back, units[i - 1])
        send(back, units[-1])
        if units[0] == 0:
            returned[:parcel_rows, :] = result[:parcel_rows, :]

    for units in LANDINGS:
        await_units(back, units)
        for u in units:
            unpack(returned, rows, u)
        if units == LANDINGS[0]:
            early = (units[-1] + 1) * SLOTS

            @spread
            def _(at):
                mixed_ref[:, at] = jnp.dot(
                    place[:, :early], rows[:early, at], preferred_element_type=F32
                ).astype(BF16)

    @spread
    def _(at):
        late = jnp.dot(place[:, early:], rows[early:, at], preferred_element_type=F32)
        mixed_ref[:, at] = (mixed_ref[:, at].astype(F32) + late).astype(BF16)

    there(1, DEVICES - 1).wait_send()
    back(1, DEVICES - 1).wait_send()


def shards(tokens, expert_of, w_gate, w_up, w_down):
    count, width = tokens.shape
    hidden = w_gate.shape[2]
    slots = DEVICES * CAP
    packed = pltpu.VMEM((slots * CUT, WIDE), BF16)
    hbm = pl.BlockSpec(memory_space=pltpu.HBM)
    vmem = pl.BlockSpec(memory_space=pltpu.VMEM)
    return pl.pallas_call(
        kernel,
        out_shape=jax.ShapeDtypeStruct((count, width), BF16),
        in_specs=[hbm, hbm, hbm, hbm, hbm],
        out_specs=vmem,
        scratch_shapes=[
            pltpu.VMEM((1, count), jnp.int32),
            pltpu.VMEM((count, width), BF16),
            pltpu.VMEM((width, hidden), BF16),
            pltpu.VMEM((width, hidden), BF16),
            pltpu.VMEM((hidden, width), BF16),
            pltpu.VMEM((slots, width), BF16),
            pltpu.VMEM((slots, hidden), BF16),
            pltpu.VMEM((count, slots), BF16),
            pltpu.VMEM((CUT * CUT, CUT * CUT), BF16),
            packed, packed, packed, packed,
            pltpu.SemaphoreType.DMA,
            pltpu.SemaphoreType.DMA,
            pltpu.SemaphoreType.DMA((3,)),
            pltpu.SemaphoreType.DMA,
            pltpu.SemaphoreType.DMA((len(GROUPS),)),
            pltpu.SemaphoreType.DMA,
            pltpu.SemaphoreType.DMA((len(LANDINGS),)),
        ],
        compiler_params=pltpu.CompilerParams(
            collective_id=0, has_side_effects=True, vmem_limit_bytes=50 * 1024 * 1024
        ),
        name="expert_exchange",
    )(expert_of.reshape(1, count), tokens, w_gate, w_up, w_down)


def solution(mesh):
    rows = P(("pair", "ep"), None)
    blocks = P(("pair", "ep"), None, None)
    return jax.shard_map(
        shards, mesh=mesh, in_specs=(rows, rows, blocks, blocks, blocks), out_specs=rows,
        check_vma=False,
    )
```

```python
import random

import jax
import jax.numpy as jnp
from jax import lax
from jax.experimental import pallas as pl
from jax.experimental.pallas import tpu as pltpu
from jax.sharding import PartitionSpec as P

MESH = pl.DeviceIdType.MESH
BF16 = jnp.bfloat16
F32 = jnp.float32

DEVICES = 128
CAP = 3
CUT, WIDE = 16, 256
UNIT = 16
SLOTS = UNIT * CAP
BLOCKS = SLOTS // CUT
UNITS = DEVICES // UNIT
GROUPS = ((0, 1, 2, 3), (4, 5, 6, 7))
LANDINGS = ((0, 1, 2, 3), (4, 5, 6), (7,))
AHEAD = 3
SPREAD = 1024


def split(off):
    return off // 32, (off // 16) % 2, (off // 4) % 4, off % 4


def distance(off):
    dx, _, dz, dy = split(off)
    return sum(min(d, 4 - d) for d in (dx, dz, dy))


def even_order():
    def hops(off):
        dx, _, dz, dy = split(off)
        return [int(d in way) for d in (dx, dz, dy) for way in ((1, 2), (3, 2))]

    def spread_of(off):
        total = [a + b for a, b in zip(load, hops(off))]
        return sum(t * t for t in total) * len(total) - sum(total) ** 2

    rng = random.Random(1)
    rest, load, order = list(range(1, DEVICES)), [0] * 6, [0]
    while rest:
        rng.shuffle(rest)
        best = min(rest, key=spread_of)
        rest.remove(best)
        load = [a + b for a, b in zip(load, hops(best))]
        order.append(best)
    return order


ORDER = even_order()


def step_of(expert, x, core, z, y):
    dx = (expert // 32 + 4 - x) % 4
    dc = ((expert // 16) % 2 + core) % 2
    dz = ((expert // 4) % 4 + 4 - z) % 4
    dy = (expert % 4 + 4 - y) % 4
    off = dx * 32 + dc * 16 + dz * 4 + dy
    step = jnp.zeros_like(off)
    for k, met in enumerate(ORDER):
        step = jnp.where(off == met, k, step)
    return step


def kernel(
    expert_hbm, tok_hbm, wg_hbm, wu_hbm, wd_hbm, mixed_ref,
    expert, tok, wg, wu, wd, rows, hid, place, turn, outgoing, parcel, result, returned,
    expert_sem, tok_sem, w_sem, send_sem, there_sem, back_send_sem, back_sem,
):
    pair, ep = lax.axis_index("pair"), lax.axis_index("ep")
    x, core, z, y = pair // 2, pair % 2, ep // 4, ep % 4
    pairs = [((x + d // 2) % 4) * 2 + (core + d % 2) % 2 for d in range(8)]
    eps = [((z + d // 4) % 4) * 4 + (y + d % 4) % 4 for d in range(16)]

    def peer(step, sign):
        dx, dc, dz, dy = split(ORDER[step])
        return pairs[(sign * dx) % 4 * 2 + dc], eps[(sign * dz) % 4 * 4 + (sign * dy) % 4]

    expert_copy = pltpu.make_async_copy(expert_hbm, expert, expert_sem)
    expert_copy.start()
    tok_copy = pltpu.make_async_copy(tok_hbm, tok, tok_sem)
    tok_copy.start()
    barrier = pltpu.get_barrier_semaphore()
    for k in sorted(range(1, DEVICES), key=lambda k: -distance(ORDER[k])):
        pl.semaphore_signal(barrier, inc=1, device_id=peer(k, 1), device_id_type=MESH)

    count = tok.shape[0]
    expert_copy.wait()
    row = expert[...]
    down = lax.broadcasted_iota(jnp.int32, (count, count), 0)
    across = lax.broadcasted_iota(jnp.int32, (count, count), 1)
    column = jnp.sum(jnp.where(down == across, row, 0), axis=1, keepdims=True)
    same = column == row
    row_rank = jnp.sum(jnp.where(same & (down < across), 1, 0), axis=0, keepdims=True)
    row_slot = step_of(row, x, core, z, y) * CAP + row_rank
    n = CUT * CUT
    turn_row = lax.broadcasted_iota(jnp.int32, (n, n), 0)
    turn_col = lax.broadcasted_iota(jnp.int32, (n, n), 1)
    turn[...] = jnp.where(
        (turn_row // CUT == turn_col % CUT) & (turn_row % CUT == turn_col // CUT), 1.0, 0.0
    ).astype(BF16)

    def pack(src, dst, unit):
        for b in range(unit * BLOCKS, (unit + 1) * BLOCKS):
            cut = jnp.concatenate(
                [src[b * CUT : (b + 1) * CUT, c * WIDE : (c + 1) * WIDE] for c in range(CUT)],
                axis=0,
            )
            turned = jnp.dot(turn[...], cut, preferred_element_type=F32).astype(BF16)
            dst[b * n : (b + 1) * n, :] = turned

    def unpack(src, dst, unit):
        for b in range(unit * BLOCKS, (unit + 1) * BLOCKS):
            cut = src[b * n : (b + 1) * n, :]
            turned = jnp.dot(turn[...], cut, preferred_element_type=F32).astype(BF16)
            for c in range(CUT):
                dst[b * CUT : (b + 1) * CUT, c * WIDE : (c + 1) * WIDE] = turned[
                    c * CUT : (c + 1) * CUT, :
                ]

    def spread(body):
        @pl.loop(0, tok.shape[1] // SPREAD)
        def _(c):
            body(pl.ds(pl.multiple_of(c * SPREAD, SPREAD), SPREAD))

    parcel_rows = CAP * CUT

    def span(step, steps=1):
        return pl.ds(step * parcel_rows, steps * parcel_rows)

    def there(k, steps=1):
        return pltpu.make_async_remote_copy(
            src_ref=outgoing.at[span(k, steps)], dst_ref=parcel.at[span(k, steps)],
            send_sem=send_sem, recv_sem=there_sem.at[[k // UNIT in g for g in GROUPS].index(True)],
            device_id=peer(k, 1), device_id_type=MESH,
        )

    def back(k, steps=1):
        return pltpu.make_async_remote_copy(
            src_ref=result.at[span(k, steps)], dst_ref=returned.at[span(k, steps)],
            send_sem=back_send_sem,
            recv_sem=back_sem.at[[k // UNIT in g for g in LANDINGS].index(True)],
            device_id=peer(k, -1), device_id_type=MESH,
        )

    def send(copy, unit):
        for k in range(max(unit * UNIT, 1), (unit + 1) * UNIT):
            copy(k).start()

    def await_units(copy, units):
        lo = max(units[0] * UNIT, 1)
        copy(lo, (units[-1] + 1) * UNIT - lo).wait_recv()

    def select(unit):
        pick = jnp.where(
            lax.broadcasted_iota(jnp.int32, (SLOTS, count), 0) + unit * SLOTS == row_slot, 1.0, 0.0
        ).astype(BF16)

        @spread
        def _(at):
            rows[unit * SLOTS : (unit + 1) * SLOTS, at] = jnp.dot(
                pick, tok[:, at], preferred_element_type=F32
            ).astype(BF16)

    tok_copy.wait()
    for u in range(UNITS):
        select(u)
        pack(rows, outgoing, u)
        if u == AHEAD - 1:
            pl.semaphore_wait(barrier, DEVICES - 1)
            for v in range(AHEAD - 1):
                send(there, v)
        if u >= AHEAD:
            send(there, u - 1)
    send(there, UNITS - 1)
    parcel[:parcel_rows, :] = outgoing[:parcel_rows, :]

    w_copies = [
        pltpu.make_async_copy(src.at[0], dst, w_sem.at[i])
        for i, (src, dst) in enumerate(((wg_hbm, wg), (wu_hbm, wu), (wd_hbm, wd)))
    ]
    for copy in w_copies:
        copy.start()

    col_slot = jnp.sum(jnp.where(down == across, row_slot, 0), axis=1, keepdims=True)
    place[...] = jnp.where(
        lax.broadcasted_iota(jnp.int32, (count, DEVICES * CAP), 1) == col_slot, 1.0, 0.0
    ).astype(BF16)
    for copy in w_copies:
        copy.wait()

    for units in GROUPS:
        await_units(there, units)
        for u in units:
            unpack(parcel, rows, u)
        held = slice(units[0] * SLOTS, (units[-1] + 1) * SLOTS)
        for j in range(0, wg.shape[1], WIDE):
            arrived = rows[held, :]
            gate = jnp.dot(arrived, wg[:, j : j + WIDE], preferred_element_type=F32)
            up = jnp.dot(arrived, wu[:, j : j + WIDE], preferred_element_type=F32)
            hid[held, j : j + WIDE] = (gate / (1.0 + jnp.exp(-gate)) * up).astype(BF16)

        @spread
        def _(at):
            rows[held, at] = jnp.dot(hid[held, :], wd[:, at], preferred_element_type=F32).astype(BF16)

        for i, u in enumerate(units):
            pack(rows, result, u)
            if i:
                send(back, units[i - 1])
        send(back, units[-1])
        if units[0] == 0:
            returned[:parcel_rows, :] = result[:parcel_rows, :]

    for units in LANDINGS:
        await_units(back, units)
        for u in units:
            unpack(returned, rows, u)
        if units == LANDINGS[-2]:
            early = (units[-1] + 1) * SLOTS

            @spread
            def _(at):
                mixed_ref[:, at] = jnp.dot(
                    place[:, :early], rows[:early, at], preferred_element_type=F32
                ).astype(BF16)

    @spread
    def _(at):
        late = jnp.dot(place[:, early:], rows[early:, at], preferred_element_type=F32)
        mixed_ref[:, at] = (mixed_ref[:, at].astype(F32) + late).astype(BF16)

    there(1, DEVICES - 1).wait_send()
    back(1, DEVICES - 1).wait_send()


def shards(tokens, expert_of, w_gate, w_up, w_down):
    count, width = tokens.shape
    hidden = w_gate.shape[2]
    slots = DEVICES * CAP
    packed = pltpu.VMEM((slots * CUT, WIDE), BF16)
    hbm = pl.BlockSpec(memory_space=pltpu.HBM)
    vmem = pl.BlockSpec(memory_space=pltpu.VMEM)
    return pl.pallas_call(
        kernel,
        out_shape=jax.ShapeDtypeStruct((count, width), BF16),
        in_specs=[hbm, hbm, hbm, hbm, hbm],
        out_specs=vmem,
        scratch_shapes=[
            pltpu.VMEM((1, count), jnp.int32),
            pltpu.VMEM((count, width), BF16),
            pltpu.VMEM((width, hidden), BF16),
            pltpu.VMEM((width, hidden), BF16),
            pltpu.VMEM((hidden, width), BF16),
            pltpu.VMEM((slots, width), BF16),
            pltpu.VMEM((slots, hidden), BF16),
            pltpu.VMEM((count, slots), BF16),
            pltpu.VMEM((CUT * CUT, CUT * CUT), BF16),
            packed, packed, packed, packed,
            pltpu.SemaphoreType.DMA,
            pltpu.SemaphoreType.DMA,
            pltpu.SemaphoreType.DMA((3,)),
            pltpu.SemaphoreType.DMA,
            pltpu.SemaphoreType.DMA((len(GROUPS),)),
            pltpu.SemaphoreType.DMA,
            pltpu.SemaphoreType.DMA((len(LANDINGS),)),
        ],
        compiler_params=pltpu.CompilerParams(
            collective_id=0, has_side_effects=True, vmem_limit_bytes=50 * 1024 * 1024
        ),
        name="expert_exchange",
    )(pltpu.with_memory_space_constraint(expert_of.reshape(1, count), pltpu.HBM), tokens, w_gate, w_up, w_down)


def solution(mesh):
    rows = P(("pair", "ep"), None)
    blocks = P(("pair", "ep"), None, None)
    return jax.shard_map(
        shards, mesh=mesh, in_specs=(rows, rows, blocks, blocks, blocks), out_specs=rows,
        check_vma=False,
    )
```

```python
import random

import jax
import jax.numpy as jnp
from jax import lax
from jax.experimental import pallas as pl
from jax.experimental.pallas import tpu as pltpu
from jax.sharding import PartitionSpec as P

MESH = pl.DeviceIdType.MESH
BF16 = jnp.bfloat16
F32 = jnp.float32

DEVICES = 128
CAP = 3
CUT, WIDE = 16, 256
UNIT = 16
SLOTS = UNIT * CAP
BLOCKS = SLOTS // CUT
UNITS = DEVICES // UNIT
GROUPS = ((0, 1, 2, 3), (4, 5, 6, 7))
LANDINGS = ((0, 1, 2, 3), (4, 5, 6), (7,))
NEAR, PLANES = 20, 48
SPREAD = 1024


def split(off):
    return off // 32, (off // 16) % 2, (off // 4) % 4, off % 4


def distance(off):
    dx, _, dz, dy = split(off)
    return sum(min(d, 4 - d) for d in (dx, dz, dy))


def turns(off):
    dx, _, dz, dy = split(off)
    return (dx > 0) + (dz > 0) + (dy > 0)


def even_order():
    def hops(off):
        dx, _, dz, dy = split(off)
        return [int(d in way) for d in (dx, dz, dy) for way in ((1, 2), (3, 2))]

    def spread_of(off):
        total = [a + b for a, b in zip(load, hops(off))]
        return sum(t * t for t in total) * len(total) - sum(total) ** 2

    rng = random.Random(1)
    rest, load, order = list(range(1, DEVICES)), [0] * 6, [0]
    while rest:
        rng.shuffle(rest)
        far = 1 if len(order) < NEAR else 2 if len(order) < PLANES else 3
        best = min((off for off in rest if turns(off) <= far), key=spread_of)
        rest.remove(best)
        load = [a + b for a, b in zip(load, hops(best))]
        order.append(best)
    return order


ORDER = even_order()


def step_of(expert, x, core, z, y):
    dx = (expert // 32 + 4 - x) % 4
    dc = ((expert // 16) % 2 + core) % 2
    dz = ((expert // 4) % 4 + 4 - z) % 4
    dy = (expert % 4 + 4 - y) % 4
    off = dx * 32 + dc * 16 + dz * 4 + dy
    step = jnp.zeros_like(off)
    for k, met in enumerate(ORDER):
        step = jnp.where(off == met, k, step)
    return step


def kernel(
    expert_hbm, tok_hbm, wg_hbm, wu_hbm, wd_hbm, mixed_ref,
    expert, tok, wg, wu, wd, rows, hid, place, turn, outgoing, parcel, result, returned,
    expert_sem, tok_sem, w_sem, send_sem, there_sem, back_send_sem, back_sem,
    planes_sem, all_sem,
):
    pair, ep = lax.axis_index("pair"), lax.axis_index("ep")
    x, core, z, y = pair // 2, pair % 2, ep // 4, ep % 4
    pairs = [((x + d // 2) % 4) * 2 + (core + d % 2) % 2 for d in range(8)]
    eps = [((z + d // 4) % 4) * 4 + (y + d % 4) % 4 for d in range(16)]

    def peer(step, sign):
        dx, dc, dz, dy = split(ORDER[step])
        return pairs[(sign * dx) % 4 * 2 + dc], eps[(sign * dz) % 4 * 4 + (sign * dy) % 4]

    expert_copy = pltpu.make_async_copy(expert_hbm, expert, expert_sem)
    expert_copy.start()
    tok_copy = pltpu.make_async_copy(tok_hbm, tok, tok_sem)
    tok_copy.start()
    barrier = pltpu.get_barrier_semaphore()
    for k in range(1, NEAR):
        pl.semaphore_signal(barrier, inc=1, device_id=peer(k, 1), device_id_type=MESH)

    count = tok.shape[0]
    expert_copy.wait()
    row = expert[...]
    down = lax.broadcasted_iota(jnp.int32, (count, count), 0)
    across = lax.broadcasted_iota(jnp.int32, (count, count), 1)
    column = jnp.sum(jnp.where(down == across, row, 0), axis=1, keepdims=True)
    same = column == row
    row_rank = jnp.sum(jnp.where(same & (down < across), 1, 0), axis=0, keepdims=True)
    row_slot = step_of(row, x, core, z, y) * CAP + row_rank
    n = CUT * CUT
    turn_row = lax.broadcasted_iota(jnp.int32, (n, n), 0)
    turn_col = lax.broadcasted_iota(jnp.int32, (n, n), 1)
    turn[...] = jnp.where(
        (turn_row // CUT == turn_col % CUT) & (turn_row % CUT == turn_col // CUT), 1.0, 0.0
    ).astype(BF16)

    def pack(src, dst, unit):
        for b in range(unit * BLOCKS, (unit + 1) * BLOCKS):
            cut = jnp.concatenate(
                [src[b * CUT : (b + 1) * CUT, c * WIDE : (c + 1) * WIDE] for c in range(CUT)],
                axis=0,
            )
            turned = jnp.dot(turn[...], cut, preferred_element_type=F32).astype(BF16)
            dst[b * n : (b + 1) * n, :] = turned

    def unpack(src, dst, unit):
        for b in range(unit * BLOCKS, (unit + 1) * BLOCKS):
            cut = src[b * n : (b + 1) * n, :]
            turned = jnp.dot(turn[...], cut, preferred_element_type=F32).astype(BF16)
            for c in range(CUT):
                dst[b * CUT : (b + 1) * CUT, c * WIDE : (c + 1) * WIDE] = turned[
                    c * CUT : (c + 1) * CUT, :
                ]

    def spread(body):
        @pl.loop(0, tok.shape[1] // SPREAD)
        def _(c):
            body(pl.ds(pl.multiple_of(c * SPREAD, SPREAD), SPREAD))

    parcel_rows = CAP * CUT

    def span(step, steps=1):
        return pl.ds(step * parcel_rows, steps * parcel_rows)

    def there(k, steps=1):
        return pltpu.make_async_remote_copy(
            src_ref=outgoing.at[span(k, steps)], dst_ref=parcel.at[span(k, steps)],
            send_sem=send_sem, recv_sem=there_sem.at[[k // UNIT in g for g in GROUPS].index(True)],
            device_id=peer(k, 1), device_id_type=MESH,
        )

    def back(k, steps=1):
        return pltpu.make_async_remote_copy(
            src_ref=result.at[span(k, steps)], dst_ref=returned.at[span(k, steps)],
            send_sem=back_send_sem,
            recv_sem=back_sem.at[[k // UNIT in g for g in LANDINGS].index(True)],
            device_id=peer(k, -1), device_id_type=MESH,
        )

    def send(copy, unit):
        for k in range(max(unit * UNIT, 1), (unit + 1) * UNIT):
            copy(k).start()

    def await_units(copy, units):
        lo = max(units[0] * UNIT, 1)
        copy(lo, (units[-1] + 1) * UNIT - lo).wait_recv()

    def select(unit):
        pick = jnp.where(
            lax.broadcasted_iota(jnp.int32, (SLOTS, count), 0) + unit * SLOTS == row_slot, 1.0, 0.0
        ).astype(BF16)

        @spread
        def _(at):
            rows[unit * SLOTS : (unit + 1) * SLOTS, at] = jnp.dot(
                pick, tok[:, at], preferred_element_type=F32
            ).astype(BF16)

    tok_copy.wait()
    def tell(sem, offs):
        for off in offs:
            pl.semaphore_signal(
                sem, inc=1, device_id=peer(ORDER.index(off), 1), device_id_type=MESH
            )

    for u in range(UNITS):
        select(u)
        pack(rows, outgoing, u)
        if u == 0:
            pl.semaphore_wait(barrier, NEAR - 1)
            tell(planes_sem, [d * 4 for d in (1, 2, 3)] + [1, 2, 3])
        elif u == 1:
            send(there, 0)
            pl.semaphore_wait(planes_sem, 6)
            tell(all_sem, [d * 32 for d in (1, 2, 3)])
        else:
            send(there, u - 1)
            if u * UNIT == PLANES:
                pl.semaphore_wait(all_sem, 3)
    send(there, UNITS - 1)
    parcel[:parcel_rows, :] = outgoing[:parcel_rows, :]

    w_copies = [
        pltpu.make_async_copy(src.at[0], dst, w_sem.at[i])
        for i, (src, dst) in enumerate(((wg_hbm, wg), (wu_hbm, wu), (wd_hbm, wd)))
    ]
    for copy in w_copies:
        copy.start()

    col_slot = jnp.sum(jnp.where(down == across, row_slot, 0), axis=1, keepdims=True)
    place[...] = jnp.where(
        lax.broadcasted_iota(jnp.int32, (count, DEVICES * CAP), 1) == col_slot, 1.0, 0.0
    ).astype(BF16)
    for copy in w_copies:
        copy.wait()

    for units in GROUPS:
        await_units(there, units)
        for u in units:
            unpack(parcel, rows, u)
        held = slice(units[0] * SLOTS, (units[-1] + 1) * SLOTS)
        for j in range(0, wg.shape[1], WIDE):
            arrived = rows[held, :]
            gate = jnp.dot(arrived, wg[:, j : j + WIDE], preferred_element_type=F32)
            up = jnp.dot(arrived, wu[:, j : j + WIDE], preferred_element_type=F32)
            hid[held, j : j + WIDE] = (gate / (1.0 + jnp.exp(-gate)) * up).astype(BF16)

        @spread
        def _(at):
            rows[held, at] = jnp.dot(hid[held, :], wd[:, at], preferred_element_type=F32).astype(BF16)

        for i, u in enumerate(units):
            pack(rows, result, u)
            if i:
                send(back, units[i - 1])
        send(back, units[-1])
        if units[0] == 0:
            returned[:parcel_rows, :] = result[:parcel_rows, :]

    for units in LANDINGS:
        await_units(back, units)
        for u in units:
            unpack(returned, rows, u)
        if units == LANDINGS[-2]:
            early = (units[-1] + 1) * SLOTS

            @spread
            def _(at):
                mixed_ref[:, at] = jnp.dot(
                    place[:, :early], rows[:early, at], preferred_element_type=F32
                ).astype(BF16)

    @spread
    def _(at):
        late = jnp.dot(place[:, early:], rows[early:, at], preferred_element_type=F32)
        mixed_ref[:, at] = (mixed_ref[:, at].astype(F32) + late).astype(BF16)

    there(1, DEVICES - 1).wait_send()
    back(1, DEVICES - 1).wait_send()


def shards(tokens, expert_of, w_gate, w_up, w_down):
    count, width = tokens.shape
    hidden = w_gate.shape[2]
    slots = DEVICES * CAP
    packed = pltpu.VMEM((slots * CUT, WIDE), BF16)
    hbm = pl.BlockSpec(memory_space=pltpu.HBM)
    vmem = pl.BlockSpec(memory_space=pltpu.VMEM)
    return pl.pallas_call(
        kernel,
        out_shape=jax.ShapeDtypeStruct((count, width), BF16),
        in_specs=[hbm, hbm, hbm, hbm, hbm],
        out_specs=vmem,
        scratch_shapes=[
            pltpu.VMEM((1, count), jnp.int32),
            pltpu.VMEM((count, width), BF16),
            pltpu.VMEM((width, hidden), BF16),
            pltpu.VMEM((width, hidden), BF16),
            pltpu.VMEM((hidden, width), BF16),
            pltpu.VMEM((slots, width), BF16),
            pltpu.VMEM((slots, hidden), BF16),
            pltpu.VMEM((count, slots), BF16),
            pltpu.VMEM((CUT * CUT, CUT * CUT), BF16),
            packed, packed, packed, packed,
            pltpu.SemaphoreType.DMA,
            pltpu.SemaphoreType.DMA,
            pltpu.SemaphoreType.DMA((3,)),
            pltpu.SemaphoreType.DMA,
            pltpu.SemaphoreType.DMA((len(GROUPS),)),
            pltpu.SemaphoreType.DMA,
            pltpu.SemaphoreType.DMA((len(LANDINGS),)),
            pltpu.SemaphoreType.REGULAR,
            pltpu.SemaphoreType.REGULAR,
        ],
        compiler_params=pltpu.CompilerParams(
            collective_id=0, has_side_effects=True, vmem_limit_bytes=50 * 1024 * 1024
        ),
        name="expert_exchange",
    )(pltpu.with_memory_space_constraint(expert_of.reshape(1, count), pltpu.HBM), tokens, w_gate, w_up, w_down)


def solution(mesh):
    rows = P(("pair", "ep"), None)
    blocks = P(("pair", "ep"), None, None)
    return jax.shard_map(
        shards, mesh=mesh, in_specs=(rows, rows, blocks, blocks, blocks), out_specs=rows,
        check_vma=False,
    )
```

```python
import random

import jax
import jax.numpy as jnp
from jax import lax
from jax.experimental import pallas as pl
from jax.experimental.pallas import tpu as pltpu
from jax.sharding import PartitionSpec as P

MESH = pl.DeviceIdType.MESH
BF16 = jnp.bfloat16
F32 = jnp.float32

DEVICES = 128
CAP = 3
CUT, WIDE = 16, 256
UNIT = 16
SLOTS = UNIT * CAP
BLOCKS = SLOTS // CUT
UNITS = DEVICES // UNIT
GROUPS = ((0, 1), (2, 3), (4, 5), (6, 7))
LANDINGS = ((0, 1, 2, 3), (4, 5), (6,), (7,))
NEAR, PLANES = 20, 48
SPREAD = 1024


def split(off):
    return off // 32, (off // 16) % 2, (off // 4) % 4, off % 4


def distance(off):
    dx, _, dz, dy = split(off)
    return sum(min(d, 4 - d) for d in (dx, dz, dy))


def turns(off):
    dx, _, dz, dy = split(off)
    return (dx > 0) + (dz > 0) + (dy > 0)


def even_order():
    def hops(off):
        dx, _, dz, dy = split(off)
        return [int(d in way) for d in (dx, dz, dy) for way in ((1, 2), (3, 2))]

    def spread_of(off):
        total = [a + b for a, b in zip(load, hops(off))]
        return sum(t * t for t in total) * len(total) - sum(total) ** 2

    rng = random.Random(1)
    rest, load, order = list(range(1, DEVICES)), [0] * 6, [0]
    while rest:
        rng.shuffle(rest)
        far = 1 if len(order) < NEAR else 2 if len(order) < PLANES else 3
        best = min((off for off in rest if turns(off) <= far), key=spread_of)
        rest.remove(best)
        load = [a + b for a, b in zip(load, hops(best))]
        order.append(best)
    return order


ORDER = even_order()


def step_of(expert, x, core, z, y):
    dx = (expert // 32 + 4 - x) % 4
    dc = ((expert // 16) % 2 + core) % 2
    dz = ((expert // 4) % 4 + 4 - z) % 4
    dy = (expert % 4 + 4 - y) % 4
    off = dx * 32 + dc * 16 + dz * 4 + dy
    step = jnp.zeros_like(off)
    for k, met in enumerate(ORDER):
        step = jnp.where(off == met, k, step)
    return step


def kernel(
    expert_hbm, tok_hbm, wg_hbm, wu_hbm, wd_hbm, mixed_ref,
    expert, tok, wg, wu, wd, rows, hid, place, turn, outgoing, parcel, result, returned,
    expert_sem, tok_sem, w_sem, send_sem, there_sem, back_send_sem, back_sem,
    planes_sem, all_sem,
):
    pair, ep = lax.axis_index("pair"), lax.axis_index("ep")
    x, core, z, y = pair // 2, pair % 2, ep // 4, ep % 4
    pairs = [((x + d // 2) % 4) * 2 + (core + d % 2) % 2 for d in range(8)]
    eps = [((z + d // 4) % 4) * 4 + (y + d % 4) % 4 for d in range(16)]

    def peer(step, sign):
        dx, dc, dz, dy = split(ORDER[step])
        return pairs[(sign * dx) % 4 * 2 + dc], eps[(sign * dz) % 4 * 4 + (sign * dy) % 4]

    expert_copy = pltpu.make_async_copy(expert_hbm, expert, expert_sem)
    expert_copy.start()
    tok_copy = pltpu.make_async_copy(tok_hbm, tok, tok_sem)
    tok_copy.start()
    barrier = pltpu.get_barrier_semaphore()
    for k in range(1, NEAR):
        pl.semaphore_signal(barrier, inc=1, device_id=peer(k, 1), device_id_type=MESH)

    n = CUT * CUT
    turn_row = lax.broadcasted_iota(jnp.int32, (n, n), 0)
    turn_col = lax.broadcasted_iota(jnp.int32, (n, n), 1)
    turn[...] = jnp.where(
        (turn_row // CUT == turn_col % CUT) & (turn_row % CUT == turn_col // CUT), 1.0, 0.0
    ).astype(BF16)

    count = tok.shape[0]
    down = lax.broadcasted_iota(jnp.int32, (count, count), 0)
    across = lax.broadcasted_iota(jnp.int32, (count, count), 1)
    earlier = jnp.where(down < across, 1.0, 0.0).astype(BF16)
    expert_copy.wait()
    row = expert[...]
    named = lax.broadcasted_iota(jnp.int32, (DEVICES, count), 0) == row
    before = jnp.dot(
        jnp.where(named, 1.0, 0.0).astype(BF16), earlier, preferred_element_type=F32
    )
    row_rank = jnp.sum(jnp.where(named, before, 0.0), axis=0, keepdims=True).astype(jnp.int32)
    row_slot = step_of(row, x, core, z, y) * CAP + row_rank

    def pack(src, dst, unit):
        for b in range(unit * BLOCKS, (unit + 1) * BLOCKS):
            cut = jnp.concatenate(
                [src[b * CUT : (b + 1) * CUT, c * WIDE : (c + 1) * WIDE] for c in range(CUT)],
                axis=0,
            )
            turned = jnp.dot(turn[...], cut, preferred_element_type=F32).astype(BF16)
            dst[b * n : (b + 1) * n, :] = turned

    def unpack(src, dst, unit):
        for b in range(unit * BLOCKS, (unit + 1) * BLOCKS):
            cut = src[b * n : (b + 1) * n, :]
            turned = jnp.dot(turn[...], cut, preferred_element_type=F32).astype(BF16)
            for c in range(CUT):
                dst[b * CUT : (b + 1) * CUT, c * WIDE : (c + 1) * WIDE] = turned[
                    c * CUT : (c + 1) * CUT, :
                ]

    def spread(body):
        @pl.loop(0, tok.shape[1] // SPREAD)
        def _(c):
            body(pl.ds(pl.multiple_of(c * SPREAD, SPREAD), SPREAD))

    parcel_rows = CAP * CUT

    def span(step, steps=1):
        return pl.ds(step * parcel_rows, steps * parcel_rows)

    def there(k, steps=1):
        return pltpu.make_async_remote_copy(
            src_ref=outgoing.at[span(k, steps)], dst_ref=parcel.at[span(k, steps)],
            send_sem=send_sem, recv_sem=there_sem.at[[k // UNIT in g for g in GROUPS].index(True)],
            device_id=peer(k, 1), device_id_type=MESH,
        )

    def back(k, steps=1):
        return pltpu.make_async_remote_copy(
            src_ref=result.at[span(k, steps)], dst_ref=returned.at[span(k, steps)],
            send_sem=back_send_sem,
            recv_sem=back_sem.at[[k // UNIT in g for g in LANDINGS].index(True)],
            device_id=peer(k, -1), device_id_type=MESH,
        )

    def send(copy, unit):
        for k in range(max(unit * UNIT, 1), (unit + 1) * UNIT):
            copy(k).start()

    def await_units(copy, units):
        lo = max(units[0] * UNIT, 1)
        copy(lo, (units[-1] + 1) * UNIT - lo).wait_recv()

    def select(unit):
        pick = jnp.where(
            lax.broadcasted_iota(jnp.int32, (SLOTS, count), 0) + unit * SLOTS == row_slot, 1.0, 0.0
        ).astype(BF16)

        @spread
        def _(at):
            rows[unit * SLOTS : (unit + 1) * SLOTS, at] = jnp.dot(
                pick, tok[:, at], preferred_element_type=F32
            ).astype(BF16)

    tok_copy.wait()
    def tell(sem, offs):
        for off in offs:
            pl.semaphore_signal(
                sem, inc=1, device_id=peer(ORDER.index(off), 1), device_id_type=MESH
            )

    for u in range(UNITS):
        select(u)
        if u > 0:
            send(there, u - 1)
        pack(rows, outgoing, u)
        if u == 0:
            pl.semaphore_wait(barrier, NEAR - 1)
            tell(planes_sem, [d * 4 for d in (1, 2, 3)] + [1, 2, 3])
        if u == 1:
            pl.semaphore_wait(planes_sem, 6)
            tell(all_sem, [d * 32 for d in (1, 2, 3)])
        if u * UNIT == PLANES:
            pl.semaphore_wait(all_sem, 3)
    send(there, UNITS - 1)
    parcel[:parcel_rows, :] = outgoing[:parcel_rows, :]

    w_copies = [
        pltpu.make_async_copy(src.at[0], dst, w_sem.at[i])
        for i, (src, dst) in enumerate(((wg_hbm, wg), (wu_hbm, wu), (wd_hbm, wd)))
    ]
    for copy in w_copies:
        copy.start()

    col_slot = jnp.sum(jnp.where(down == across, row_slot, 0), axis=1, keepdims=True)
    place[...] = jnp.where(
        lax.broadcasted_iota(jnp.int32, (count, DEVICES * CAP), 1) == col_slot, 1.0, 0.0
    ).astype(BF16)
    for copy in w_copies:
        copy.wait()

    for units in GROUPS:
        await_units(there, units)
        for u in units:
            unpack(parcel, rows, u)
        held = slice(units[0] * SLOTS, (units[-1] + 1) * SLOTS)
        for j in range(0, wg.shape[1], WIDE):
            arrived = rows[held, :]
            gate = jnp.dot(arrived, wg[:, j : j + WIDE], preferred_element_type=F32)
            up = jnp.dot(arrived, wu[:, j : j + WIDE], preferred_element_type=F32)
            hid[held, j : j + WIDE] = (gate / (1.0 + jnp.exp(-gate)) * up).astype(BF16)

        @spread
        def _(at):
            rows[held, at] = jnp.dot(hid[held, :], wd[:, at], preferred_element_type=F32).astype(BF16)

        for i, u in enumerate(units):
            pack(rows, result, u)
            if i:
                send(back, units[i - 1])
        send(back, units[-1])
        if units[0] == 0:
            returned[:parcel_rows, :] = result[:parcel_rows, :]

    for units in LANDINGS:
        await_units(back, units)
        for u in units:
            unpack(returned, rows, u)
        if units == LANDINGS[0]:
            early = (units[-1] + 1) * SLOTS

            @spread
            def _(at):
                mixed_ref[:, at] = jnp.dot(
                    place[:, :early], rows[:early, at], preferred_element_type=F32
                ).astype(BF16)

    for c in range(0, tok.shape[1], SPREAD):
        at = slice(c, c + SPREAD)
        late = jnp.dot(place[:, early:], rows[early:, at], preferred_element_type=F32)
        mixed_ref[:, at] = (mixed_ref[:, at].astype(F32) + late).astype(BF16)

    there(1, DEVICES - 1).wait_send()
    back(1, DEVICES - 1).wait_send()


def shards(tokens, expert_of, w_gate, w_up, w_down):
    count, width = tokens.shape
    hidden = w_gate.shape[2]
    slots = DEVICES * CAP
    packed = pltpu.VMEM((slots * CUT, WIDE), BF16)
    hbm = pl.BlockSpec(memory_space=pltpu.HBM)
    vmem = pl.BlockSpec(memory_space=pltpu.VMEM)
    return pl.pallas_call(
        kernel,
        out_shape=jax.ShapeDtypeStruct((count, width), BF16),
        in_specs=[hbm, hbm, hbm, hbm, hbm],
        out_specs=vmem,
        scratch_shapes=[
            pltpu.VMEM((1, count), jnp.int32),
            pltpu.VMEM((count, width), BF16),
            pltpu.VMEM((width, hidden), BF16),
            pltpu.VMEM((width, hidden), BF16),
            pltpu.VMEM((hidden, width), BF16),
            pltpu.VMEM((slots, width), BF16),
            pltpu.VMEM((slots, hidden), BF16),
            pltpu.VMEM((count, slots), BF16),
            pltpu.VMEM((CUT * CUT, CUT * CUT), BF16),
            packed, packed, packed, packed,
            pltpu.SemaphoreType.DMA,
            pltpu.SemaphoreType.DMA,
            pltpu.SemaphoreType.DMA((3,)),
            pltpu.SemaphoreType.DMA,
            pltpu.SemaphoreType.DMA((len(GROUPS),)),
            pltpu.SemaphoreType.DMA,
            pltpu.SemaphoreType.DMA((len(LANDINGS),)),
            pltpu.SemaphoreType.REGULAR,
            pltpu.SemaphoreType.REGULAR,
        ],
        compiler_params=pltpu.CompilerParams(
            collective_id=0, has_side_effects=True, vmem_limit_bytes=50 * 1024 * 1024
        ),
        name="expert_exchange",
    )(pltpu.with_memory_space_constraint(expert_of.reshape(1, count), pltpu.HBM), tokens, w_gate, w_up, w_down)


def solution(mesh):
    rows = P(("pair", "ep"), None)
    blocks = P(("pair", "ep"), None, None)
    return jax.shard_map(
        shards, mesh=mesh, in_specs=(rows, rows, blocks, blocks, blocks), out_specs=rows,
        check_vma=False,
    )
```

```python
import random

import jax
import jax.numpy as jnp
from jax import lax
from jax.experimental import pallas as pl
from jax.experimental.pallas import tpu as pltpu
from jax.sharding import PartitionSpec as P

MESH = pl.DeviceIdType.MESH
BF16 = jnp.bfloat16
F32 = jnp.float32

DEVICES = 128
CAP = 3
CUT, WIDE = 16, 256
UNIT = 16
SLOTS = UNIT * CAP
BLOCKS = SLOTS // CUT
UNITS = DEVICES // UNIT
GROUPS = ((0, 1), (2, 3), (4, 5), (6, 7))
LANDINGS = ((0, 1, 2, 3), (4, 5), (6,), (7,))
NEAR, PLANES = 20, 32
SPREAD = 1024


def split(off):
    return off // 32, (off // 16) % 2, (off // 4) % 4, off % 4


def distance(off):
    dx, _, dz, dy = split(off)
    return sum(min(d, 4 - d) for d in (dx, dz, dy))


def turns(off):
    dx, _, dz, dy = split(off)
    return (dx > 0) + (dz > 0) + (dy > 0)


def even_order():
    def hops(off):
        dx, _, dz, dy = split(off)
        return [int(d in way) for d in (dx, dz, dy) for way in ((1, 2), (3, 2))]

    def spread_of(off):
        total = [a + b for a, b in zip(load, hops(off))]
        return sum(t * t for t in total) * len(total) - sum(total) ** 2

    rng = random.Random(1)
    rest, load, order = list(range(1, DEVICES)), [0] * 6, [0]
    while rest:
        rng.shuffle(rest)
        far = 1 if len(order) < NEAR else 2 if len(order) < PLANES else 3
        best = min((off for off in rest if turns(off) <= far), key=spread_of)
        rest.remove(best)
        load = [a + b for a, b in zip(load, hops(best))]
        order.append(best)
    return order


ORDER = even_order()


def step_of(expert, x, core, z, y):
    dx = (expert // 32 + 4 - x) % 4
    dc = ((expert // 16) % 2 + core) % 2
    dz = ((expert // 4) % 4 + 4 - z) % 4
    dy = (expert % 4 + 4 - y) % 4
    off = dx * 32 + dc * 16 + dz * 4 + dy
    step = jnp.zeros_like(off)
    for k, met in enumerate(ORDER):
        step = jnp.where(off == met, k, step)
    return step


def kernel(
    expert_hbm, tok_hbm, wg_hbm, wu_hbm, wd_hbm, mixed_ref,
    expert, tok, wg, wu, wd, rows, hid, place, turn, outgoing, parcel, result, returned,
    expert_sem, tok_sem, w_sem, send_sem, there_sem, back_send_sem, back_sem,
    planes_sem, all_sem,
):
    pair, ep = lax.axis_index("pair"), lax.axis_index("ep")
    x, core, z, y = pair // 2, pair % 2, ep // 4, ep % 4
    pairs = [((x + d // 2) % 4) * 2 + (core + d % 2) % 2 for d in range(8)]
    eps = [((z + d // 4) % 4) * 4 + (y + d % 4) % 4 for d in range(16)]

    def peer(step, sign):
        dx, dc, dz, dy = split(ORDER[step])
        return pairs[(sign * dx) % 4 * 2 + dc], eps[(sign * dz) % 4 * 4 + (sign * dy) % 4]

    expert_copy = pltpu.make_async_copy(expert_hbm, expert, expert_sem)
    expert_copy.start()
    tok_copy = pltpu.make_async_copy(tok_hbm, tok, tok_sem)
    tok_copy.start()
    barrier = pltpu.get_barrier_semaphore()
    for k in range(1, NEAR):
        pl.semaphore_signal(barrier, inc=1, device_id=peer(k, 1), device_id_type=MESH)

    n = CUT * CUT
    turn_row = lax.broadcasted_iota(jnp.int32, (n, n), 0)
    turn_col = lax.broadcasted_iota(jnp.int32, (n, n), 1)
    turn[...] = jnp.where(
        (turn_row // CUT == turn_col % CUT) & (turn_row % CUT == turn_col // CUT), 1.0, 0.0
    ).astype(BF16)

    count = tok.shape[0]
    down = lax.broadcasted_iota(jnp.int32, (count, count), 0)
    across = lax.broadcasted_iota(jnp.int32, (count, count), 1)
    earlier = jnp.where(down < across, 1.0, 0.0).astype(BF16)
    expert_copy.wait()
    row = expert[...]
    named = lax.broadcasted_iota(jnp.int32, (DEVICES, count), 0) == row
    before = jnp.dot(
        jnp.where(named, 1.0, 0.0).astype(BF16), earlier, preferred_element_type=F32
    )
    row_rank = jnp.sum(jnp.where(named, before, 0.0), axis=0, keepdims=True).astype(jnp.int32)
    row_slot = step_of(row, x, core, z, y) * CAP + row_rank

    def pack(src, dst, unit):
        for b in range(unit * BLOCKS, (unit + 1) * BLOCKS):
            cut = jnp.concatenate(
                [src[b * CUT : (b + 1) * CUT, c * WIDE : (c + 1) * WIDE] for c in range(CUT)],
                axis=0,
            )
            turned = jnp.dot(turn[...], cut, preferred_element_type=F32).astype(BF16)
            dst[b * n : (b + 1) * n, :] = turned

    def unpack(src, dst, unit):
        for b in range(unit * BLOCKS, (unit + 1) * BLOCKS):
            cut = src[b * n : (b + 1) * n, :]
            turned = jnp.dot(turn[...], cut, preferred_element_type=F32).astype(BF16)
            for c in range(CUT):
                dst[b * CUT : (b + 1) * CUT, c * WIDE : (c + 1) * WIDE] = turned[
                    c * CUT : (c + 1) * CUT, :
                ]

    def spread(body):
        @pl.loop(0, tok.shape[1] // SPREAD)
        def _(c):
            body(pl.ds(pl.multiple_of(c * SPREAD, SPREAD), SPREAD))

    parcel_rows = CAP * CUT

    def span(step, steps=1):
        return pl.ds(step * parcel_rows, steps * parcel_rows)

    def there(k, steps=1):
        return pltpu.make_async_remote_copy(
            src_ref=outgoing.at[span(k, steps)], dst_ref=parcel.at[span(k, steps)],
            send_sem=send_sem, recv_sem=there_sem.at[[k // UNIT in g for g in GROUPS].index(True)],
            device_id=peer(k, 1), device_id_type=MESH,
        )

    def back(k, steps=1):
        return pltpu.make_async_remote_copy(
            src_ref=result.at[span(k, steps)], dst_ref=returned.at[span(k, steps)],
            send_sem=back_send_sem,
            recv_sem=back_sem.at[[k // UNIT in g for g in LANDINGS].index(True)],
            device_id=peer(k, -1), device_id_type=MESH,
        )

    def send(copy, unit):
        for k in range(max(unit * UNIT, 1), (unit + 1) * UNIT):
            copy(k).start()

    def await_units(copy, units):
        lo = max(units[0] * UNIT, 1)
        copy(lo, (units[-1] + 1) * UNIT - lo).wait_recv()

    def select(unit):
        pick = jnp.where(
            lax.broadcasted_iota(jnp.int32, (SLOTS, count), 0) + unit * SLOTS == row_slot, 1.0, 0.0
        ).astype(BF16)

        @spread
        def _(at):
            rows[unit * SLOTS : (unit + 1) * SLOTS, at] = jnp.dot(
                pick, tok[:, at], preferred_element_type=F32
            ).astype(BF16)

    tok_copy.wait()
    def tell(sem, offs):
        for off in offs:
            pl.semaphore_signal(
                sem, inc=1, device_id=peer(ORDER.index(off), 1), device_id_type=MESH
            )

    for u in range(UNITS):
        select(u)
        if u > 0:
            send(there, u - 1)
        pack(rows, outgoing, u)
        if u == 0:
            pl.semaphore_wait(barrier, NEAR - 1)
            tell(planes_sem, [d * 4 for d in (1, 2, 3)] + [1, 2, 3])
        if u == 1:
            pl.semaphore_wait(planes_sem, 6)
            tell(all_sem, [d * 32 for d in (1, 2, 3)])
        if u * UNIT == PLANES:
            pl.semaphore_wait(all_sem, 3)
    send(there, UNITS - 1)
    parcel[:parcel_rows, :] = outgoing[:parcel_rows, :]

    w_copies = [
        pltpu.make_async_copy(src.at[0], dst, w_sem.at[i])
        for i, (src, dst) in enumerate(((wg_hbm, wg), (wu_hbm, wu), (wd_hbm, wd)))
    ]
    for copy in w_copies:
        copy.start()

    col_slot = jnp.sum(jnp.where(down == across, row_slot, 0), axis=1, keepdims=True)
    place[...] = jnp.where(
        lax.broadcasted_iota(jnp.int32, (count, DEVICES * CAP), 1) == col_slot, 1.0, 0.0
    ).astype(BF16)
    for copy in w_copies:
        copy.wait()

    for units in GROUPS:
        await_units(there, units)
        for u in units:
            unpack(parcel, rows, u)
        held = slice(units[0] * SLOTS, (units[-1] + 1) * SLOTS)
        for j in range(0, wg.shape[1], WIDE):
            arrived = rows[held, :]
            gate = jnp.dot(arrived, wg[:, j : j + WIDE], preferred_element_type=F32)
            up = jnp.dot(arrived, wu[:, j : j + WIDE], preferred_element_type=F32)
            hid[held, j : j + WIDE] = (gate / (1.0 + jnp.exp(-gate)) * up).astype(BF16)

        @spread
        def _(at):
            rows[held, at] = jnp.dot(hid[held, :], wd[:, at], preferred_element_type=F32).astype(BF16)

        for i, u in enumerate(units):
            pack(rows, result, u)
            if i:
                send(back, units[i - 1])
        send(back, units[-1])
        if units[0] == 0:
            returned[:parcel_rows, :] = result[:parcel_rows, :]

    for units in LANDINGS:
        await_units(back, units)
        for u in units:
            unpack(returned, rows, u)
        if units == LANDINGS[0]:
            early = (units[-1] + 1) * SLOTS

            @spread
            def _(at):
                mixed_ref[:, at] = jnp.dot(
                    place[:, :early], rows[:early, at], preferred_element_type=F32
                ).astype(BF16)

    for c in range(0, tok.shape[1], SPREAD):
        at = slice(c, c + SPREAD)
        late = jnp.dot(place[:, early:], rows[early:, at], preferred_element_type=F32)
        mixed_ref[:, at] = (mixed_ref[:, at].astype(F32) + late).astype(BF16)

    there(1, DEVICES - 1).wait_send()
    back(1, DEVICES - 1).wait_send()


def shards(tokens, expert_of, w_gate, w_up, w_down):
    count, width = tokens.shape
    hidden = w_gate.shape[2]
    slots = DEVICES * CAP
    packed = pltpu.VMEM((slots * CUT, WIDE), BF16)
    hbm = pl.BlockSpec(memory_space=pltpu.HBM)
    vmem = pl.BlockSpec(memory_space=pltpu.VMEM)
    return pl.pallas_call(
        kernel,
        out_shape=jax.ShapeDtypeStruct((count, width), BF16),
        in_specs=[hbm, hbm, hbm, hbm, hbm],
        out_specs=vmem,
        scratch_shapes=[
            pltpu.VMEM((1, count), jnp.int32),
            pltpu.VMEM((count, width), BF16),
            pltpu.VMEM((width, hidden), BF16),
            pltpu.VMEM((width, hidden), BF16),
            pltpu.VMEM((hidden, width), BF16),
            pltpu.VMEM((slots, width), BF16),
            pltpu.VMEM((slots, hidden), BF16),
            pltpu.VMEM((count, slots), BF16),
            pltpu.VMEM((CUT * CUT, CUT * CUT), BF16),
            packed, packed, packed, packed,
            pltpu.SemaphoreType.DMA,
            pltpu.SemaphoreType.DMA,
            pltpu.SemaphoreType.DMA((3,)),
            pltpu.SemaphoreType.DMA,
            pltpu.SemaphoreType.DMA((len(GROUPS),)),
            pltpu.SemaphoreType.DMA,
            pltpu.SemaphoreType.DMA((len(LANDINGS),)),
            pltpu.SemaphoreType.REGULAR,
            pltpu.SemaphoreType.REGULAR,
        ],
        compiler_params=pltpu.CompilerParams(
            collective_id=0, has_side_effects=True, vmem_limit_bytes=50 * 1024 * 1024
        ),
        name="expert_exchange",
    )(pltpu.with_memory_space_constraint(expert_of.reshape(1, count), pltpu.HBM), tokens, w_gate, w_up, w_down)


def solution(mesh):
    rows = P(("pair", "ep"), None)
    blocks = P(("pair", "ep"), None, None)
    return jax.shard_map(
        shards, mesh=mesh, in_specs=(rows, rows, blocks, blocks, blocks), out_specs=rows,
        check_vma=False,
    )
```
